32 devices in a mesh: frag: 2 (over y), band: 8 (over z, x), slab: 2 (over core).
Axes of the slice: x: 2, y: 2, z: 4, core: 2. Of those that a mesh axis runs over, the one named last changes fastest.
Arguments:
- wavefunctions: bfloat16 [2048, 16384], P('band', ('frag', 'slab')), parts along dimension 1, may hold values from -6 to 6
- eigvec: bfloat16 [2048, 4096], P(None, ('frag', 'band', 'slab')), parts along dimension 1, may hold values from -1 to 1, as said below
- occupation: float32 [4096], P('frag'), parts along dimension 0, may hold values from 0.1 to 2
Outputs:
- rotated: float32 [2048, 16384], P('band', ('frag', 'slab')), parts along dimension 1
- density: float32 [16384], P(('frag', 'slab')), parts along dimension 0
The draws below stay inside these ranges and needn't reach their ends.
There are 2 independent parts, one for each index of `frag`. The reference program is written for one: setup_inputs(seed, part) draws one part's arguments, and reference() takes and returns one part's arrays. A program takes and returns all parts, laid end to end along the dimension named above; each array names one. Nothing has to cross between parts.
Inputs may be any that keep to these rules, and one draw needn't show every extreme that they name: eigvec is an orthogonal matrix rounded to bfloat16.
All inputs are finite; a program needn't handle non-finite values.
Results may differ from the reference program's by a relative error of at most 0.0003.
Values may be sent and summed in bfloat16 or wider, within the bound.
A program may use at most 64 MiB of HBM per device.

```python
import math
import jax
import jax.numpy as jnp

NB = 2048
NPTS = 8192


def draw_eigvec(key, part):
    sample = jax.random.normal(jax.random.fold_in(key, 7), (NB, NB), jnp.float32)
    basis, upper = jnp.linalg.qr(sample)
    signs = jnp.where(jnp.diagonal(upper) < 0, -1.0, 1.0).astype(jnp.float32)
    return (basis * signs[None, :]).astype(jnp.bfloat16)


def level_of(rng, shape, pieces, low, largest):
    loudness = 1.0
    for dim, shards_of in pieces:
        draws = jax.random.uniform(jax.random.fold_in(jax.random.fold_in(rng, 6), dim), (shards_of,), jnp.float32, low / len(pieces), largest / len(pieces))
        loudness = loudness * jnp.repeat(jnp.exp(draws), shape[dim] // shards_of).reshape((-1,) + (1,) * (len(shape) - 1 - dim))
    return loudness


def normal_values(rng, dims, deviation, limit, cuts=(), held_as=jnp.bfloat16):
    values = deviation * jax.random.normal(rng, dims, jnp.float32)
    if cuts:
        values = values * level_of(rng, dims, cuts, -0.22, 0.18)
    return jnp.clip(values, -limit, limit).astype(held_as)


def setup_inputs(seed: int = 0, part: int = 0) -> dict:
    arg_keys = jax.random.split(jax.random.key(seed), 4)
    part_keys = jax.random.split(jax.random.fold_in(arg_keys[3], part), 4)
    return {
        "wavefunctions": normal_values(part_keys[0], (NB, NPTS), 1.0, 6.0, ((0, 8), (1, 2))),
        "eigvec": draw_eigvec(jax.random.fold_in(jax.random.fold_in(arg_keys[3], part), 71), part),
        "occupation": jnp.clip(jnp.exp(jax.random.uniform(part_keys[2], (NB,), jnp.float32, math.log(0.1), math.log(2.0))), 0.1, 2.0),
    }


def reference(wavefunctions, eigvec, occupation):
    rotated = jnp.dot(eigvec.T.astype(jnp.float32), wavefunctions.astype(jnp.float32), preferred_element_type=jnp.float32)
    weighted = occupation[:, None] * rotated * rotated
    density = jnp.sum(weighted, axis=0) / jnp.float32(NB)
    return (rotated, density)
```

```python
import functools

import jax
import jax.numpy as jnp
from jax import lax
from jax.experimental import pallas as pl
from jax.experimental.pallas import tpu as pltpu
from jax.sharding import PartitionSpec as P

MESH = pl.DeviceIdType.MESH
LANES = 128
AHEAD = 5


def plain(wavefunctions, eigvec, occupation):
    total_bands = eigvec.shape[0]
    by_points = lax.all_to_all(wavefunctions, "band", split_axis=1, concat_axis=0, tiled=True)
    point_rows = lax.dot_general(
        lax.all_gather(eigvec, ("band", "slab"), axis=1, tiled=True),
        by_points,
        (((0,), (0,)), ((), ())),
        preferred_element_type=jnp.float32,
    )
    rotated = lax.all_to_all(point_rows, "band", split_axis=0, concat_axis=1, tiled=True)
    local_density = jnp.dot(
        occupation,
        point_rows * point_rows,
        precision=lax.Precision.HIGHEST,
        preferred_element_type=jnp.float32,
    ) / jnp.float32(total_bands)
    density = lax.all_gather(local_density, "band", axis=0, tiled=True)
    return (rotated, density)


def kernel(nb, wave, panel, weight, out, density, gathered, vectors, staged, part, parts, zrecv, up, down, xrecv, xsend, own, erecv, esend, orecv, osend, drecv, dsend):
    nz = nb // 2
    frag, band, slab = (lax.axis_index(name) for name in ("frag", "band", "slab"))
    z, x = band // 2, lax.rem(band, 2)
    rows, points = wave.shape
    half = points // 2
    steps = half // LANES
    width = panel.shape[0]
    total_bands = panel.shape[1]

    def at(b, s=slab):
        return (frag, b, s)

    beside = 2 * z + 1 - x
    above, below = lax.rem(band + 2, nb), lax.rem(band + nb - 2, nb)

    barrier = pltpu.get_barrier_semaphore()
    for hop in range(1, nb):
        pl.semaphore_signal(barrier, inc=1, device_id=at(lax.rem(band + hop, nb)), device_id_type=MESH)
    for target in (at(band, 1 - slab), at(beside, 1 - slab)):
        pl.semaphore_signal(barrier, inc=1, device_id=target, device_id_type=MESH)
    pl.semaphore_wait(barrier, nb + 1)

    def send(src, dst, ssem, rsem, target):
        return pltpu.make_async_remote_copy(
            src_ref=src, dst_ref=dst, send_sem=ssem, recv_sem=rsem, device_id=target, device_id_type=MESH
        )

    def columns(of, step):
        return pl.ds(pl.multiple_of(of * half + step * LANES, LANES), LANES)

    mine = vectors.at[pl.ds(pl.multiple_of((2 * x + slab) * width, width), width)]

    def vector_copy(i, target):
        return send(panel, mine, esend.at[i], erecv.at[2 * x + slab], target)

    def vector_from(x2, s2):
        there = vectors.at[pl.ds(pl.multiple_of((2 * x2 + s2) * width, width), width)]
        return send(there, there, esend.at[0], erecv.at[2 * x2 + s2], at(band, 1 - slab))

    def across(step):
        return send(wave.at[:, columns(1 - x, step)], gathered.at[step, band], xsend.at[step], xrecv.at[step], at(beside))

    def across_from(step):
        there = gathered.at[step, beside]
        return send(there, there, xsend.at[step], xrecv.at[step], at(beside))

    def keep(step):
        return pltpu.make_async_copy(wave.at[:, columns(x, step)], gathered.at[step, band], own.at[step])

    def pair(step, origin, sems, target):
        both = gathered.at[step, pl.ds(2 * origin, 2)]
        return send(both, both, sems.at[step, origin], zrecv.at[step, origin], at(target))

    def result(step):
        return send(staged.at[step], out.at[:, columns(x, step)], osend.at[step], orecv.at[step], at(beside))

    def result_from(step):
        there = out.at[:, columns(1 - x, step)]
        return send(there, there, osend.at[step], orecv.at[step], at(beside))

    copies = [
        vector_copy(0, at(band, 1 - slab)),
        vector_copy(1, at(beside)),
        vector_copy(2, at(beside, 1 - slab)),
    ]

    def begin(step, _):
        across(step).start()
        keep(step).start()
        return _

    lax.fori_loop(0, AHEAD, begin, 0)
    for copy in copies:
        copy.start()
    home = pltpu.make_async_copy(panel, mine, own.at[steps])
    home.start()
    lax.fori_loop(AHEAD, steps, begin, 0)

    def spread(step):
        keep(step).wait()
        across_from(step).wait_recv()

        @pl.when(z < nz - 1)
        def _():
            pair(step, z, up, above).start()

        @pl.when(z > 0)
        def _():
            pair(step, z, down, below).start()

    def collect(step):
        for distance in range(1, nz):
            @pl.when(z + distance < nz)
            def _():
                pair(step, z + distance, down, above).wait_recv()

                @pl.when(z > 0)
                def _():
                    pair(step, z + distance, down, below).start()

            @pl.when(z - distance >= 0)
            def _():
                pair(step, z - distance, up, below).wait_recv()

                @pl.when(z < nz - 1)
                def _():
                    pair(step, z - distance, up, above).start()

    def compute(step):
        block = gathered[step].reshape(nb * rows, LANES)
        here, there = rows * x, rows * (1 - x)
        kept = jnp.dot(vectors[pl.ds(pl.multiple_of(here, rows), rows), :], block, preferred_element_type=jnp.float32)
        sent = jnp.dot(vectors[pl.ds(pl.multiple_of(there, rows), rows), :], block, preferred_element_type=jnp.float32)
        staged[step] = sent
        out[:, columns(x, step)] = kept
        sums = jnp.sum(weight[pl.ds(pl.multiple_of(here, rows), rows), :] * kept * kept, axis=0, keepdims=True)
        sums = sums + jnp.sum(weight[pl.ds(pl.multiple_of(there, rows), rows), :] * sent * sent, axis=0, keepdims=True)
        part[0, :, pl.ds(pl.multiple_of(step * LANES, LANES), LANES)] = sums
        result(step).start()

    def first(step, carry):
        spread(step)
        return carry

    lax.fori_loop(0, AHEAD, first, 0)
    home.wait()
    for hop in range(1, 4):
        x2 = x if hop == 1 else 1 - x
        s2 = slab if hop == 2 else 1 - slab
        vector_from(x2, s2).wait_recv()

    def body(step, carry):
        @pl.when(step + AHEAD < steps)
        def _():
            spread(step + AHEAD)

        collect(step)
        compute(step)
        return carry

    lax.fori_loop(0, steps, body, 0)

    def share(hop):
        target = lax.rem(band + hop, nb)
        return send(part.at[0], parts.at[band], dsend.at[hop], drecv.at[band], at(target))

    for hop in range(1, nb):
        share(hop).start()
    parts[band] = part[0]

    def finish(step, carry):
        result_from(step).wait_recv()
        result(step).wait_send()
        across(step).wait_send()
        for origin in range(nz):
            @pl.when((z < nz - 1) & (origin <= z))
            def _():
                pair(step, origin, up, above).wait_send()

            @pl.when((z > 0) & (origin >= z))
            def _():
                pair(step, origin, down, below).wait_send()

        return carry

    lax.fori_loop(0, steps, finish, 0)
    for copy in copies:
        copy.wait_send()
    for hop in range(1, nb):
        share(hop).wait_send()
        source = lax.rem(band + nb - hop, nb)
        send(parts.at[source], parts.at[source], dsend.at[hop], drecv.at[source], at(source)).wait_recv()
    for side in range(2):
        total = parts[side]
        for level in range(1, nz):
            total = total + parts[2 * level + side]
        density[side] = total / jnp.float32(total_bands)


def local(nb, wavefunctions, eigvec, occupation):
    rows, points = wavefunctions.shape
    total_bands, width = eigvec.shape
    if nb % 2 or width % LANES or rows != 2 * width or points % (2 * LANES) or points // 2 // LANES <= AHEAD:
        return plain(wavefunctions, eigvec, occupation)
    nz, half = nb // 2, points // 2
    steps = half // LANES
    weights = lax.dynamic_slice(occupation, (lax.axis_index("band") // 2 * (2 * rows),), (2 * rows,))
    weights = jnp.broadcast_to(weights[:, None], (2 * rows, LANES))
    vmem = pl.BlockSpec(memory_space=pltpu.VMEM)
    dma = pltpu.SemaphoreType.DMA
    rotated, density = pl.pallas_call(
        functools.partial(kernel, nb),
        out_shape=(
            jax.ShapeDtypeStruct((rows, points), jnp.float32),
            jax.ShapeDtypeStruct((2, 1, half), jnp.float32),
        ),
        in_specs=[vmem] * 3,
        out_specs=(vmem, vmem),
        scratch_shapes=[
            pltpu.VMEM((steps, nb, rows, LANES), jnp.bfloat16),
            pltpu.VMEM((2 * rows, total_bands), jnp.bfloat16),
            pltpu.VMEM((steps, rows, LANES), jnp.float32),
            pltpu.VMEM((1, 1, half), jnp.float32),
            pltpu.VMEM((nb, 1, half), jnp.float32),
            dma((steps, nz)),
            dma((steps, nz)),
            dma((steps, nz)),
            dma((steps,)),
            dma((steps,)),
            dma((steps + 1,)),
            dma((4,)),
            dma((3,)),
            dma((steps,)),
            dma((steps,)),
            dma((nb,)),
            dma((nb,)),
        ],
        compiler_params=pltpu.CompilerParams(
            collective_id=0, has_side_effects=True, vmem_limit_bytes=56 * 2**20
        ),
    )(wavefunctions, eigvec.T, weights)
    return (rotated, density.reshape(points))


def solution(mesh):
    placed = (P("band", ("frag", "slab")), P(None, ("frag", "band", "slab")), P("frag"))
    return jax.shard_map(
        functools.partial(local, mesh.shape["band"]),
        mesh=mesh,
        in_specs=placed,
        out_specs=(P("band", ("frag", "slab")), P(("frag", "slab"))),
        check_vma=False,
    )
```

```python
import functools

import jax
import jax.numpy as jnp
from jax import lax
from jax.experimental import pallas as pl
from jax.experimental.pallas import tpu as pltpu
from jax.sharding import PartitionSpec as P

MESH = pl.DeviceIdType.MESH
LANES = 128
AHEAD = 10


def plain(wavefunctions, eigvec, occupation):
    total_bands = eigvec.shape[0]
    by_points = lax.all_to_all(wavefunctions, "band", split_axis=1, concat_axis=0, tiled=True)
    point_rows = lax.dot_general(
        lax.all_gather(eigvec, ("band", "slab"), axis=1, tiled=True),
        by_points,
        (((0,), (0,)), ((), ())),
        preferred_element_type=jnp.float32,
    )
    rotated = lax.all_to_all(point_rows, "band", split_axis=0, concat_axis=1, tiled=True)
    local_density = jnp.dot(
        occupation,
        point_rows * point_rows,
        precision=lax.Precision.HIGHEST,
        preferred_element_type=jnp.float32,
    ) / jnp.float32(total_bands)
    density = lax.all_gather(local_density, "band", axis=0, tiled=True)
    return (rotated, density)


def kernel(nb, wave, panel, weight, out, density, gathered, vectors, staged, part, parts, zrecv, up, down, xrecv, xsend, own, erecv, esend, orecv, osend, drecv, dsend):
    nz = nb // 2
    frag, band, slab = (lax.axis_index(name) for name in ("frag", "band", "slab"))
    z, x = band // 2, lax.rem(band, 2)
    rows, points = wave.shape
    half = points // 2
    steps = half // LANES
    width = panel.shape[0]
    total_bands = panel.shape[1]

    def at(b, s=slab):
        return (frag, b, s)

    beside = 2 * z + 1 - x
    above, below = lax.rem(band + 2, nb), lax.rem(band + nb - 2, nb)

    barrier = pltpu.get_barrier_semaphore()
    for hop in range(1, nb):
        pl.semaphore_signal(barrier, inc=1, device_id=at(lax.rem(band + hop, nb)), device_id_type=MESH)
    for target in (at(band, 1 - slab), at(beside, 1 - slab)):
        pl.semaphore_signal(barrier, inc=1, device_id=target, device_id_type=MESH)
    pl.semaphore_wait(barrier, nb + 1)

    def send(src, dst, ssem, rsem, target):
        return pltpu.make_async_remote_copy(
            src_ref=src, dst_ref=dst, send_sem=ssem, recv_sem=rsem, device_id=target, device_id_type=MESH
        )

    def columns(of, step):
        return pl.ds(pl.multiple_of(of * half + step * LANES, LANES), LANES)

    mine = vectors.at[pl.ds(pl.multiple_of((2 * x + slab) * width, width), width)]

    def vector_copy(i, target):
        return send(panel, mine, esend.at[i], erecv.at[2 * x + slab], target)

    def vector_from(x2, s2):
        there = vectors.at[pl.ds(pl.multiple_of((2 * x2 + s2) * width, width), width)]
        return send(there, there, esend.at[0], erecv.at[2 * x2 + s2], at(band, 1 - slab))

    def across(step):
        return send(wave.at[:, columns(1 - x, step)], gathered.at[step, band], xsend.at[step], xrecv.at[step], at(beside))

    def across_from(step):
        there = gathered.at[step, beside]
        return send(there, there, xsend.at[step], xrecv.at[step], at(beside))

    def keep(step):
        return pltpu.make_async_copy(wave.at[:, columns(x, step)], gathered.at[step, band], own.at[step])

    def pair(step, origin, sems, target):
        both = gathered.at[step, pl.ds(2 * origin, 2)]
        return send(both, both, sems.at[step, origin], zrecv.at[step, origin], at(target))

    def result(step):
        return send(staged.at[step], out.at[:, columns(x, step)], osend.at[step], orecv.at[step], at(beside))

    def result_from(step):
        there = out.at[:, columns(1 - x, step)]
        return send(there, there, osend.at[step], orecv.at[step], at(beside))

    copies = [
        vector_copy(0, at(band, 1 - slab)),
        vector_copy(1, at(beside)),
    ]
    passed = vectors.at[pl.ds(pl.multiple_of((2 * (1 - x) + slab) * width, width), width)]
    relay = send(passed, passed, esend.at[2], erecv.at[2 * (1 - x) + slab], at(band, 1 - slab))

    def begin(step, _):
        across(step).start()
        keep(step).start()
        return _

    lax.fori_loop(0, AHEAD, begin, 0)
    for copy in copies:
        copy.start()
    home = pltpu.make_async_copy(panel, mine, own.at[steps])
    home.start()
    lax.fori_loop(AHEAD, steps, begin, 0)

    def spread(step):
        keep(step).wait()
        across_from(step).wait_recv()

        @pl.when(z < nz - 1)
        def _():
            pair(step, z, up, above).start()

        @pl.when(z > 0)
        def _():
            pair(step, z, down, below).start()

    def collect(step):
        for distance in range(1, nz):
            @pl.when(z + distance < nz)
            def _():
                pair(step, z + distance, down, above).wait_recv()

                @pl.when(z > 0)
                def _():
                    pair(step, z + distance, down, below).start()

            @pl.when(z - distance >= 0)
            def _():
                pair(step, z - distance, up, below).wait_recv()

                @pl.when(z < nz - 1)
                def _():
                    pair(step, z - distance, up, above).start()

    def compute(step):
        block = gathered[step].reshape(nb * rows, LANES)
        here, there = rows * x, rows * (1 - x)
        kept = jnp.dot(vectors[pl.ds(pl.multiple_of(here, rows), rows), :], block, preferred_element_type=jnp.float32)
        sent = jnp.dot(vectors[pl.ds(pl.multiple_of(there, rows), rows), :], block, preferred_element_type=jnp.float32)
        staged[step] = sent
        out[:, columns(x, step)] = kept
        sums = jnp.sum(weight[pl.ds(pl.multiple_of(here, rows), rows), :] * kept * kept, axis=0, keepdims=True)
        sums = sums + jnp.sum(weight[pl.ds(pl.multiple_of(there, rows), rows), :] * sent * sent, axis=0, keepdims=True)
        part[0, :, pl.ds(pl.multiple_of(step * LANES, LANES), LANES)] = sums
        result(step).start()

    def first(step, carry):
        spread(step)
        return carry

    lax.fori_loop(0, AHEAD, first, 0)
    home.wait()
    vector_from(1 - x, slab).wait_recv()
    relay.start()
    vector_from(x, 1 - slab).wait_recv()
    vector_from(1 - x, 1 - slab).wait_recv()

    def body(step, carry):
        @pl.when(step + AHEAD < steps)
        def _():
            spread(step + AHEAD)

        collect(step)
        compute(step)
        return carry

    lax.fori_loop(0, steps, body, 0)

    def share(hop):
        target = lax.rem(band + hop, nb)
        return send(part.at[0], parts.at[band], dsend.at[hop], drecv.at[band], at(target))

    for hop in range(1, nb):
        share(hop).start()
    parts[band] = part[0]

    def finish(step, carry):
        result_from(step).wait_recv()
        result(step).wait_send()
        across(step).wait_send()
        for origin in range(nz):
            @pl.when((z < nz - 1) & (origin <= z))
            def _():
                pair(step, origin, up, above).wait_send()

            @pl.when((z > 0) & (origin >= z))
            def _():
                pair(step, origin, down, below).wait_send()

        return carry

    lax.fori_loop(0, steps, finish, 0)
    for copy in (*copies, relay):
        copy.wait_send()
    for hop in range(1, nb):
        share(hop).wait_send()
        source = lax.rem(band + nb - hop, nb)
        send(parts.at[source], parts.at[source], dsend.at[hop], drecv.at[source], at(source)).wait_recv()
    for side in range(2):
        total = parts[side]
        for level in range(1, nz):
            total = total + parts[2 * level + side]
        density[side] = total / jnp.float32(total_bands)


def local(nb, wavefunctions, eigvec, occupation):
    rows, points = wavefunctions.shape
    total_bands, width = eigvec.shape
    if nb % 2 or width % LANES or rows != 2 * width or points % (2 * LANES) or points // 2 // LANES <= AHEAD:
        return plain(wavefunctions, eigvec, occupation)
    nz, half = nb // 2, points // 2
    steps = half // LANES
    weights = lax.dynamic_slice(occupation, (lax.axis_index("band") // 2 * (2 * rows),), (2 * rows,))
    weights = jnp.broadcast_to(weights[:, None], (2 * rows, LANES))
    vmem = pl.BlockSpec(memory_space=pltpu.VMEM)
    dma = pltpu.SemaphoreType.DMA
    rotated, density = pl.pallas_call(
        functools.partial(kernel, nb),
        out_shape=(
            jax.ShapeDtypeStruct((rows, points), jnp.float32),
            jax.ShapeDtypeStruct((2, 1, half), jnp.float32),
        ),
        in_specs=[vmem] * 3,
        out_specs=(vmem, vmem),
        scratch_shapes=[
            pltpu.VMEM((steps, nb, rows, LANES), jnp.bfloat16),
            pltpu.VMEM((2 * rows, total_bands), jnp.bfloat16),
            pltpu.VMEM((steps, rows, LANES), jnp.float32),
            pltpu.VMEM((1, 1, half), jnp.float32),
            pltpu.VMEM((nb, 1, half), jnp.float32),
            dma((steps, nz)),
            dma((steps, nz)),
            dma((steps, nz)),
            dma((steps,)),
            dma((steps,)),
            dma((steps + 1,)),
            dma((4,)),
            dma((3,)),
            dma((steps,)),
            dma((steps,)),
            dma((nb,)),
            dma((nb,)),
        ],
        compiler_params=pltpu.CompilerParams(
            collective_id=0, has_side_effects=True, vmem_limit_bytes=56 * 2**20
        ),
    )(wavefunctions, eigvec.T, weights)
    return (rotated, density.reshape(points))


def solution(mesh):
    placed = (P("band", ("frag", "slab")), P(None, ("frag", "band", "slab")), P("frag"))
    return jax.shard_map(
        functools.partial(local, mesh.shape["band"]),
        mesh=mesh,
        in_specs=placed,
        out_specs=(P("band", ("frag", "slab")), P(("frag", "slab"))),
        check_vma=False,
    )
```
